32 devices in a mesh: act: 8 (over z, x), rep: 4 (over y, core).
Axes of the slice: x: 2, y: 2, z: 4, core: 2. Of those that a mesh axis runs over, the one named last changes fastest.
Arguments:
- estimated_returns: float32 [512, 16384], P('act', 'rep'), may hold values from -1000 to 1000
- chosen_move_ids: int32 [512, 16384], P('act', 'rep'), may hold values from 0 to 17
- previous_eta: float32 [1], replicated, may hold values from 0.3 to 3
- trust_region_epsilon: float32 [1], replicated, may hold values from 0.02 to 1
Outputs:
- sample_importance: float32 [512, 16384], P('act', 'rep')
- goal_distribution: float32 [18, 16384], P(None, ('rep', 'act'))
- new_temperature: float32 [1], replicated
The draws below stay inside these ranges and needn't reach their ends.
All inputs are finite; a program needn't handle non-finite values.
Results may differ from the reference program's by a relative error of at most 0.0003.
Values sent between devices are 32-bit elements; how exact they have to be, the bound alone decides.
A program may use at most 64 MiB of HBM per device.

```python
import math
import jax
import jax.numpy as jnp

SAMPLE_COUNT = 512
NACT = 18
ITERS = 3
STATE_DEV = 512
STATES = 16384


def draw_estimated_returns(key, part):
    key_base = jax.random.fold_in(key, 11)
    key_scale = jax.random.fold_in(key, 12)
    key_block = jax.random.fold_in(key, 13)
    key_shift = jax.random.fold_in(key, 14)
    base = jax.random.truncated_normal(key_base, -4.0, 4.0, (SAMPLE_COUNT, STATES), jnp.float32)
    scale_per_row = jnp.exp(jax.random.uniform(key_scale, (STATES,), jnp.float32, jnp.log(0.3), jnp.log(3.0)))
    block_scale = jnp.exp(jax.random.uniform(key_block, (STATES // STATE_DEV,), jnp.float32, jnp.log(0.5), jnp.log(2.0)))
    block_scale = jnp.repeat(block_scale, STATE_DEV)
    offset = jax.random.uniform(key_shift, (STATES,), jnp.float32, -5.0, 5.0)
    return base * (scale_per_row * block_scale)[None, :] + offset[None, :]


def touch_ends(result, rng, smallest, top_value):
    shape = result.shape
    spot = [jax.random.randint(jax.random.fold_in(rng, axis), (), 0, shape[axis]) for axis in range(len(shape))]
    result = result.at[tuple(spot)].set(smallest)
    longest = shape.index(max(shape))
    spot[longest] = (spot[longest] + 1) % shape[longest]
    return result.at[tuple(spot)].set(top_value)


def setup_inputs(seed: int = 0) -> dict:
    arg_keys = jax.random.split(jax.random.key(seed), 5)
    return {
        "estimated_returns": draw_estimated_returns(jax.random.fold_in(arg_keys[4], 71), 0),
        "chosen_move_ids": touch_ends(jax.random.randint(arg_keys[1], (SAMPLE_COUNT, STATES), 0, NACT), jax.random.fold_in(arg_keys[1], 1), 0, NACT - 1).astype(jnp.int32),
        "previous_eta": jnp.clip(jnp.exp(jax.random.uniform(arg_keys[2], (1,), jnp.float32, math.log(0.3), math.log(3.0))), 0.3, 3.0),
        "trust_region_epsilon": jnp.clip(jnp.exp(jax.random.uniform(arg_keys[3], (1,), jnp.float32, math.log(0.02), math.log(1.0))), 0.02, 1.0),
    }


def summary_figures(centered_returns, lagrange_eta):
    exponential_term = jnp.exp(centered_returns / lagrange_eta)
    partition_total = jnp.sum(exponential_term, axis=0)
    leading_part = jnp.sum(exponential_term * centered_returns, axis=0)
    trailing_part = jnp.sum(exponential_term * centered_returns * centered_returns, axis=0)
    return exponential_term, partition_total, leading_part, trailing_part


def reference(estimated_returns, chosen_move_ids, previous_eta, trust_region_epsilon):
    lagrange_eta = previous_eta[0]
    ceiling_term = trust_region_epsilon[0]
    centered_returns = estimated_returns - jnp.max(estimated_returns, axis=0, keepdims=True)
    for step in range(ITERS):
        exponential_term, partition_total, leading_part, trailing_part = summary_figures(centered_returns, lagrange_eta)
        entropy_gap = leading_part / (partition_total * lagrange_eta) - jnp.log(partition_total) + jnp.log(jnp.float32(SAMPLE_COUNT))
        mean_first = leading_part / partition_total
        spread = trailing_part / partition_total - mean_first * mean_first
        aggregate_relative_entropy = jnp.sum(entropy_gap) / STATES
        aggregate_deviation = jnp.sum(spread) / STATES
        change_amount = (ceiling_term - aggregate_relative_entropy) * lagrange_eta / (1.0 + aggregate_deviation / lagrange_eta)
        lagrange_eta = lagrange_eta * jnp.exp(-jnp.tanh(change_amount))
    exponential_term, partition_total, leading_part, trailing_part = summary_figures(centered_returns, lagrange_eta)
    probs = exponential_term / partition_total
    sample_importance = SAMPLE_COUNT * probs
    goal_distribution = jnp.stack([jnp.sum(jnp.where(chosen_move_ids == k, probs, 0.0), axis=0) for k in range(NACT)])
    return sample_importance, goal_distribution, jnp.reshape(lagrange_eta, (1,))
```

```python
import functools

import jax
import jax.numpy as jnp
from jax import lax
from jax.experimental import pallas as pl
from jax.experimental.pallas import tpu as pltpu
from jax.sharding import PartitionSpec as P

NACT = 18
ITERS = 3
LANES = 128
MESH = pl.DeviceIdType.MESH


def fold_lanes(x):
    total = x[:, :LANES]
    for i in range(1, x.shape[1] // LANES):
        total = total + x[:, i * LANES : (i + 1) * LANES]
    return total


def kernel(
    n, m, q_hbm, ids_hbm, eta_ref, eps_ref,
    expo_hbm, scale_ref, goal_ref, eta_out,
    q, ids, stat_src, stat_dst, pair_src, pair_dst, z_src, z_dst, goal_src, goal_dst, scale_src, scale_dst, delta,
    local_sem, stat_send, stat_recv, pair_send, pair_recv, z_sem, goal_sem, scale_sem,
):
    a, r = lax.axis_index("act"), lax.axis_index("rep")
    me = r * n + a
    devices = n * m
    rows, columns = q.shape
    width = columns // n
    samples = jnp.float32(rows * n)
    states = jnp.float32(columns * m)

    barrier = pltpu.get_barrier_semaphore()

    def greet(o, c):
        to = lax.rem(me + o, devices)
        pl.semaphore_signal(
            barrier, inc=1, device_id={"act": lax.rem(to, n), "rep": to // n}, device_id_type=MESH
        )
        return c

    lax.fori_loop(1, devices, greet, 0)
    load_q = pltpu.make_async_copy(q_hbm, q, local_sem.at[0])
    load_ids = pltpu.make_async_copy(ids_hbm, ids, local_sem.at[1])
    load_q.start()
    load_ids.start()
    load_q.wait()

    def cols(j):
        return pl.ds(pl.multiple_of(j * width, LANES), width)

    def to_peer(src, dst, send, recv, j):
        return pltpu.make_async_remote_copy(
            src_ref=src, dst_ref=dst, send_sem=send, recv_sem=recv,
            device_id={"act": j, "rep": r}, device_id_type=MESH,
        )

    def all_but_one(ref, count, sem):
        some = ref.at[pl.ds(0, count - 1)]
        pltpu.make_async_copy(some, some, sem).wait()

    eta = jnp.full((1, LANES), eta_ref[0], jnp.float32)
    eps = jnp.full((1, LANES), eps_ref[0], jnp.float32)

    def statistics(step, j, inverse):
        c = cols(j)
        if step == 0:
            block = q[:, c]
            top = jnp.max(block, axis=0, keepdims=True)
            shifted = block - top
            q[:, c] = shifted
            stat_src[step, j, 3:4, :] = top
        else:
            shifted = q[:, c]
        expo = jnp.exp(shifted * inverse)
        first = expo * shifted
        stat_src[step, j, 0:1, :] = jnp.sum(expo, axis=0, keepdims=True)
        stat_src[step, j, 1:2, :] = jnp.sum(first, axis=0, keepdims=True)
        stat_src[step, j, 2:3, :] = jnp.sum(first * shifted, axis=0, keepdims=True)

    for step in range(ITERS):
        inverse = 1.0 / eta[:, :1]
        if step == 0:
            lax.fori_loop(0, n, lambda o, c: (statistics(0, o, inverse), c)[1], 0)
            pl.semaphore_wait(barrier, devices - 1)

        def send(o, c):
            j = lax.rem(a + o, n)
            if step > 0:
                statistics(step, j, inverse)
            to_peer(
                stat_src.at[step, j], stat_dst.at[step, a], stat_send.at[step], stat_recv.at[step], j
            ).start()
            return c

        lax.fori_loop(1, n, send, 0)
        if step > 0:
            statistics(step, a, inverse)
        stat_dst[step, a] = stat_src[step, a]
        all_but_one(stat_dst.at[step], n, stat_recv.at[step])
        z_d = stat_dst[step, :, 0, :]
        c1_d = stat_dst[step, :, 1, :]
        c2_d = stat_dst[step, :, 2, :]
        if step == 0:
            top_d = stat_dst[step, :, 3, :]
            gap = top_d - jnp.max(top_d, axis=0, keepdims=True)
            delta[...] = gap
        else:
            gap = delta[...]
        e_d = jnp.exp(gap * inverse)
        z = jnp.sum(e_d * z_d, axis=0, keepdims=True)
        c1 = jnp.sum(e_d * (c1_d + gap * z_d), axis=0, keepdims=True)
        c2 = jnp.sum(e_d * (c2_d + gap * (2.0 * c1_d + gap * z_d)), axis=0, keepdims=True)
        mean = c1 / z
        kl = mean * inverse - jnp.log(z) + jnp.log(samples)
        spread = c2 / z - mean * mean
        pair_src[step, 0:1, :] = fold_lanes(kl)
        pair_src[step, 1:2, :] = fold_lanes(spread)

        def share(o, c):
            to = lax.rem(me + o, devices)
            pltpu.make_async_remote_copy(
                src_ref=pair_src.at[step], dst_ref=pair_dst.at[step, me],
                send_sem=pair_send.at[step], recv_sem=pair_recv.at[step],
                device_id={"act": lax.rem(to, n), "rep": to // n}, device_id_type=MESH,
            ).start()
            return c

        lax.fori_loop(1, devices, share, 0)
        pair_dst[step, me] = pair_src[step]
        all_but_one(pair_dst.at[step], devices, pair_recv.at[step])
        both = jnp.sum(pair_dst[step], axis=0)
        both = jnp.sum(both, axis=1, keepdims=True) / states
        k_mean = jnp.broadcast_to(both[0:1], (1, LANES))
        v_mean = jnp.broadcast_to(both[1:2], (1, LANES))
        change = (eps - k_mean) * eta / (1.0 + v_mean / eta)
        eta = eta * jnp.exp(-jnp.tanh(change))

    inverse = 1.0 / eta[:, :1]
    eta_out[...] = eta

    def weights(j):
        c = cols(j)
        expo = jnp.exp(q[:, c] * inverse)
        q[:, c] = expo
        z_src[j] = jnp.sum(expo, axis=0, keepdims=True)

    def send_z(o, c):
        j = lax.rem(a + o, n)
        weights(j)
        to_peer(z_src.at[j], z_dst.at[a], z_sem.at[0], z_sem.at[1], j).start()
        return c

    lax.fori_loop(1, n, send_z, 0)
    weights(a)
    z_dst[a] = z_src[a]
    store_expo = pltpu.make_async_copy(q, expo_hbm, local_sem.at[2])
    store_expo.start()
    load_ids.wait()

    def goals(j):
        c = cols(j)
        for i in range(width // LANES):
            sub = pl.ds(pl.multiple_of(j * width + i * LANES, LANES), LANES)
            expo, moves = q[:, sub], ids[:, sub]
            for k in range(NACT):
                goal_src[j, k : k + 1, i * LANES : (i + 1) * LANES] = jnp.sum(
                    jnp.where(moves == k, expo, 0.0), axis=0, keepdims=True
                )

    def send_goals(o, c):
        j = lax.rem(a + o, n)
        goals(j)
        to_peer(goal_src.at[j], goal_dst.at[a], goal_sem.at[0], goal_sem.at[1], j).start()
        return c

    lax.fori_loop(1, n, send_goals, 0)
    goals(a)
    goal_dst[a] = goal_src[a]

    all_but_one(z_dst, n, z_sem.at[1])
    e_d = jnp.exp(delta[...] * inverse)
    z = jnp.sum(e_d * z_dst[:, 0, :], axis=0, keepdims=True)
    part = e_d / z
    delta[...] = part
    scale_src[:, 0, :] = samples * part

    def send_scale(o, c):
        j = lax.rem(a + o, n)
        to_peer(scale_src.at[j], scale_dst.at[a], scale_sem.at[0], scale_sem.at[1], j).start()
        return c

    lax.fori_loop(1, n, send_scale, 0)
    scale_dst[a] = scale_src[a]
    all_but_one(goal_dst, n, goal_sem.at[1])
    goal_ref[...] = lax.fori_loop(
        0, n, lambda d, t: t + delta[pl.ds(d, 1), :] * goal_dst[d], jnp.zeros((NACT, width), jnp.float32)
    )
    all_but_one(scale_dst, n, scale_sem.at[1])

    def place(j, c):
        scale_ref[:, cols(j)] = scale_dst[j]
        return c

    lax.fori_loop(0, n, place, 0)
    for step in range(ITERS):
        all_but_one(stat_src.at[step], n, stat_send.at[step])
        some = pair_dst.at[step, pl.ds(0, devices - 1)]
        pltpu.make_async_copy(some, some, pair_send.at[step]).wait()
    all_but_one(z_src, n, z_sem.at[0])
    all_but_one(goal_src, n, goal_sem.at[0])
    all_but_one(scale_src, n, scale_sem.at[0])
    store_expo.wait()


def on_device(n, m, estimated_returns, chosen_move_ids, previous_eta, trust_region_epsilon):
    rows, columns = estimated_returns.shape
    width = columns // n
    f32 = jnp.float32
    anywhere = pl.BlockSpec(memory_space=pl.ANY)
    vmem = pl.BlockSpec(memory_space=pltpu.VMEM)
    smem = pl.BlockSpec(memory_space=pltpu.SMEM)
    dma = pltpu.SemaphoreType.DMA
    expo, scale, goal, eta = pl.pallas_call(
        functools.partial(kernel, n, m),
        name="dual",
        out_shape=(
            jax.ShapeDtypeStruct((rows, columns), f32),
            jax.ShapeDtypeStruct((1, columns), f32),
            jax.ShapeDtypeStruct((NACT, width), f32),
            jax.ShapeDtypeStruct((1, LANES), f32),
        ),
        in_specs=[anywhere, anywhere, smem, smem],
        out_specs=(anywhere, vmem, vmem, vmem),
        scratch_shapes=[
            pltpu.VMEM((rows, columns), f32),
            pltpu.VMEM((rows, columns), jnp.int32),
            pltpu.VMEM((ITERS, n, 4, width), f32),
            pltpu.VMEM((ITERS, n, 4, width), f32),
            pltpu.VMEM((ITERS, 2, LANES), f32),
            pltpu.VMEM((ITERS, n * m, 2, LANES), f32),
            pltpu.VMEM((n, 1, width), f32),
            pltpu.VMEM((n, 1, width), f32),
            pltpu.VMEM((n, NACT, width), f32),
            pltpu.VMEM((n, NACT, width), f32),
            pltpu.VMEM((n, 1, width), f32),
            pltpu.VMEM((n, 1, width), f32),
            pltpu.VMEM((n, width), f32),
            dma((3,)), dma((ITERS,)), dma((ITERS,)), dma((ITERS,)), dma((ITERS,)), dma((2,)), dma((2,)), dma((2,)),
        ],
        compiler_params=pltpu.CompilerParams(collective_id=0, has_side_effects=True),
    )(estimated_returns, chosen_move_ids, previous_eta, trust_region_epsilon)
    return expo * scale, goal, eta[0, :1]


def solution(mesh):
    n, m = mesh.shape["act"], mesh.shape["rep"]
    return jax.shard_map(
        functools.partial(on_device, n, m),
        mesh=mesh,
        in_specs=(P("act", "rep"), P("act", "rep"), P(), P()),
        out_specs=(P("act", "rep"), P(None, ("rep", "act")), P()),
        check_vma=False,
    )
```

```python
import functools

import jax
import jax.numpy as jnp
from jax import lax
from jax.experimental import pallas as pl
from jax.experimental.pallas import tpu as pltpu
from jax.sharding import PartitionSpec as P

NACT = 18
ITERS = 3
LANES = 128
MESH = pl.DeviceIdType.MESH


def fold_lanes(x):
    total = x[:, :LANES]
    for i in range(1, x.shape[1] // LANES):
        total = total + x[:, i * LANES : (i + 1) * LANES]
    return total


def kernel(
    n, m, q_hbm, ids_hbm, eta_ref, eps_ref,
    expo_hbm, scale_ref, goal_ref, eta_out,
    q, ids, stat_src, stat_dst, pair_src, pair_dst, pair_sent, z_src, z_dst, goal_src, goal_dst, scale_src, scale_dst, delta, parts,
    local_sem, stat_send, stat_recv, pair_send, pair_recv, z_sem, goal_sem, scale_sem,
):
    a, r = lax.axis_index("act"), lax.axis_index("rep")
    me = r * n + a
    devices = n * m
    rows, columns = q.shape
    width = columns // n
    owners, first_owner = n // 2, n // 4
    wide = columns // owners
    is_owner = jnp.logical_and(a >= first_owner, a < first_owner + owners)
    mine = lax.rem(a - first_owner + n, n)
    samples = jnp.float32(rows * n)
    states = jnp.float32(columns * m)

    barrier = pltpu.get_barrier_semaphore()

    def greet(o, c):
        to = lax.rem(me + o, devices)
        pl.semaphore_signal(
            barrier, inc=1, device_id={"act": lax.rem(to, n), "rep": to // n}, device_id_type=MESH
        )
        return c

    lax.fori_loop(1, devices, greet, 0)
    load_q = pltpu.make_async_copy(q_hbm, q, local_sem.at[0])
    load_ids = pltpu.make_async_copy(ids_hbm, ids, local_sem.at[1])
    load_q.start()
    load_ids.start()
    load_q.wait()

    def wide_cols(i):
        return pl.ds(pl.multiple_of(i * wide, LANES), wide)

    def cols(j):
        return pl.ds(pl.multiple_of(j * width, LANES), width)

    def to_peer(src, dst, send, recv, j):
        return pltpu.make_async_remote_copy(
            src_ref=src, dst_ref=dst, send_sem=send, recv_sem=recv,
            device_id={"act": j, "rep": r}, device_id_type=MESH,
        )

    def all_but_one(ref, count, sem):
        some = ref.at[pl.ds(0, count - 1)]
        pltpu.make_async_copy(some, some, sem).wait()

    eta = jnp.full((1, LANES), eta_ref[0], jnp.float32)
    eps = jnp.full((1, LANES), eps_ref[0], jnp.float32)

    def statistics(step, i, inverse):
        c = wide_cols(i)
        if step == 0:
            block = q[:, c]
            top = jnp.max(block, axis=0, keepdims=True)
            shifted = block - top
            q[:, c] = shifted
            stat_src[step, i, 3:4, :] = top
        else:
            shifted = q[:, c]
        expo = jnp.exp(shifted * inverse)
        first = expo * shifted
        stat_src[step, i, 0:1, :] = jnp.sum(expo, axis=0, keepdims=True)
        stat_src[step, i, 1:2, :] = jnp.sum(first, axis=0, keepdims=True)
        stat_src[step, i, 2:3, :] = jnp.sum(first * shifted, axis=0, keepdims=True)

    for step in range(ITERS):
        inverse = 1.0 / eta[:, :1]
        if step == 0:
            lax.fori_loop(0, owners, lambda i, c: (statistics(0, i, inverse), c)[1], 0)
            pl.semaphore_wait(barrier, devices - 1)

        def send(o, c):
            i = lax.rem(a - first_owner + n // 2 + o + n, owners)
            if step > 0:
                statistics(step, i, inverse)

            @pl.when(i + first_owner != a)
            def _():
                to_peer(
                    stat_src.at[step, i], stat_dst.at[step, a], stat_send.at[step], stat_recv.at[step],
                    i + first_owner,
                ).start()

            return c

        lax.fori_loop(0, owners, send, 0)

        @pl.when(is_owner)
        def _():
            stat_dst[step, a] = stat_src[step, mine]
            all_but_one(stat_dst.at[step], n, stat_recv.at[step])
            z_d = stat_dst[step, :, 0, :]
            c1_d = stat_dst[step, :, 1, :]
            c2_d = stat_dst[step, :, 2, :]
            if step == 0:
                top_d = stat_dst[step, :, 3, :]
                gap = top_d - jnp.max(top_d, axis=0, keepdims=True)
                delta[...] = gap
            else:
                gap = delta[...]
            e_d = jnp.exp(gap * inverse)
            z = jnp.sum(e_d * z_d, axis=0, keepdims=True)
            c1 = jnp.sum(e_d * (c1_d + gap * z_d), axis=0, keepdims=True)
            c2 = jnp.sum(e_d * (c2_d + gap * (2.0 * c1_d + gap * z_d)), axis=0, keepdims=True)
            mean = c1 / z
            kl = mean * inverse - jnp.log(z) + jnp.log(samples)
            spread = c2 / z - mean * mean
            pair_src[step, 0:1, :] = fold_lanes(kl)
            pair_src[step, 1:2, :] = fold_lanes(spread)
            slot = r * owners + mine

            def share(o, c):
                to = lax.rem(me + o, devices)
                pltpu.make_async_remote_copy(
                    src_ref=pair_src.at[step], dst_ref=pair_dst.at[step, slot],
                    send_sem=pair_send.at[step], recv_sem=pair_recv.at[step],
                    device_id={"act": lax.rem(to, n), "rep": to // n}, device_id_type=MESH,
                ).start()
                return c

            lax.fori_loop(1, devices, share, 0)
            pair_dst[step, slot] = pair_src[step]
            all_but_one(pair_dst.at[step], owners * m, pair_recv.at[step])

        @pl.when(jnp.logical_not(is_owner))
        def _():
            pltpu.make_async_copy(pair_dst.at[step], pair_dst.at[step], pair_recv.at[step]).wait()

        both = jnp.sum(pair_dst[step], axis=0)
        both = jnp.sum(both, axis=1, keepdims=True) / states
        k_mean = jnp.broadcast_to(both[0:1], (1, LANES))
        v_mean = jnp.broadcast_to(both[1:2], (1, LANES))
        change = (eps - k_mean) * eta / (1.0 + v_mean / eta)
        eta = eta * jnp.exp(-jnp.tanh(change))

    inverse = 1.0 / eta[:, :1]
    eta_out[...] = eta

    def weights(j):
        c = cols(j)
        expo = jnp.exp(q[:, c] * inverse)
        q[:, c] = expo
        z_src[j, 0:1, :] = jnp.sum(expo, axis=0, keepdims=True)
        z_src[j, 1:2, :] = stat_src[0, j * width // wide, 3:4, pl.ds(pl.multiple_of(lax.rem(j * width, wide), LANES), width)]

    def send_z(o, c):
        j = lax.rem(a + o, n)
        weights(j)
        to_peer(z_src.at[j], z_dst.at[a], z_sem.at[0], z_sem.at[1], j).start()
        return c

    lax.fori_loop(1, n, send_z, 0)
    weights(a)
    z_dst[a] = z_src[a]
    store_expo = pltpu.make_async_copy(q, expo_hbm, local_sem.at[2])
    store_expo.start()
    load_ids.wait()

    def goals(j):
        c = cols(j)
        for i in range(width // LANES):
            sub = pl.ds(pl.multiple_of(j * width + i * LANES, LANES), LANES)
            expo, moves = q[:, sub], ids[:, sub]
            for k in range(NACT):
                goal_src[j, k : k + 1, i * LANES : (i + 1) * LANES] = jnp.sum(
                    jnp.where(moves == k, expo, 0.0), axis=0, keepdims=True
                )

    def start_goals(o, c):
        j = lax.rem(a + o, n)
        to_peer(goal_src.at[j], goal_dst.at[a], goal_sem.at[0], goal_sem.at[1], j).start()
        return c

    def send_goals(o, c):
        goals(lax.rem(a + o, n))
        return start_goals(o, c)

    lax.fori_loop(1, n // 2, send_goals, 0)
    lax.fori_loop(n // 2, n + 1, lambda o, c: (goals(lax.rem(a + o, n)), c)[1], 0)
    goal_dst[a] = goal_src[a]

    all_but_one(z_dst, n, z_sem.at[1])
    top_d = z_dst[:, 1, :]
    e_d = jnp.exp((top_d - jnp.max(top_d, axis=0, keepdims=True)) * inverse)
    z = jnp.sum(e_d * z_dst[:, 0, :], axis=0, keepdims=True)
    part = e_d / z
    parts[...] = part
    scale_src[:, 0, :] = samples * part

    def send_scale(o, c):
        j = lax.rem(a + o, n)
        to_peer(scale_src.at[j], scale_dst.at[a], scale_sem.at[0], scale_sem.at[1], j).start()
        return c

    lax.fori_loop(1, n, send_scale, 0)
    lax.fori_loop(n // 2, n, start_goals, 0)
    scale_dst[a] = scale_src[a]
    all_but_one(goal_dst, n, goal_sem.at[1])
    goal_ref[...] = lax.fori_loop(
        0, n, lambda d, t: t + parts[pl.ds(d, 1), :] * goal_dst[d], jnp.zeros((NACT, width), jnp.float32)
    )
    all_but_one(scale_dst, n, scale_sem.at[1])

    def place(j, c):
        scale_ref[:, cols(j)] = scale_dst[j]
        return c

    lax.fori_loop(0, n, place, 0)
    for step in range(ITERS):

        @pl.when(is_owner)
        def _():
            all_but_one(stat_src.at[step], owners, stat_send.at[step])
            some = pair_sent.at[pl.ds(0, devices - 1)]
            pltpu.make_async_copy(some, some, pair_send.at[step]).wait()

        @pl.when(jnp.logical_not(is_owner))
        def _():
            pltpu.make_async_copy(stat_src.at[step], stat_src.at[step], stat_send.at[step]).wait()

    all_but_one(z_src, n, z_sem.at[0])
    all_but_one(goal_src, n, goal_sem.at[0])
    all_but_one(scale_src, n, scale_sem.at[0])
    store_expo.wait()


def finish(expo_ref, scale_ref, goal_ref, eta_ref, sample_hbm, goal_hbm, eta_hbm, sample, sem):
    rows, columns = sample.shape
    pieces = sem.shape[0] - 2
    tall = rows // pieces
    copies = [
        pltpu.make_async_copy(goal_ref, goal_hbm, sem.at[pieces]),
        pltpu.make_async_copy(eta_ref, eta_hbm, sem.at[pieces + 1]),
    ]
    for copy in copies:
        copy.start()
    for i in range(pieces):
        at = pl.ds(i * tall, tall)
        sample[at, :] = expo_ref[at, :] * scale_ref[...]
        copy = pltpu.make_async_copy(sample.at[at], sample_hbm.at[at], sem.at[i])
        copy.start()
        copies.append(copy)
    for copy in copies:
        copy.wait()


def on_device(n, m, estimated_returns, chosen_move_ids, previous_eta, trust_region_epsilon):
    rows, columns = estimated_returns.shape
    width = columns // n
    owners = n // 2
    wide = columns // owners
    f32 = jnp.float32
    anywhere = pl.BlockSpec(memory_space=pl.ANY)
    vmem = pl.BlockSpec(memory_space=pltpu.VMEM)
    smem = pl.BlockSpec(memory_space=pltpu.SMEM)
    dma = pltpu.SemaphoreType.DMA
    expo, scale, goal, eta = pl.pallas_call(
        functools.partial(kernel, n, m),
        name="dual",
        out_shape=(
            jax.ShapeDtypeStruct((rows, columns), f32),
            jax.ShapeDtypeStruct((1, columns), f32),
            jax.ShapeDtypeStruct((NACT, width), f32),
            jax.ShapeDtypeStruct((1, LANES), f32),
        ),
        in_specs=[anywhere, anywhere, smem, smem],
        out_specs=(anywhere, vmem, vmem, vmem),
        scratch_shapes=[
            pltpu.VMEM((rows, columns), f32),
            pltpu.VMEM((rows, columns), jnp.int32),
            pltpu.VMEM((ITERS, owners, 4, wide), f32),
            pltpu.VMEM((ITERS, n, 4, wide), f32),
            pltpu.VMEM((ITERS, 2, LANES), f32),
            pltpu.VMEM((ITERS, owners * m, 2, LANES), f32),
            pltpu.VMEM((n * m, 2, LANES), f32),
            pltpu.VMEM((n, 2, width), f32),
            pltpu.VMEM((n, 2, width), f32),
            pltpu.VMEM((n, NACT, width), f32),
            pltpu.VMEM((n, NACT, width), f32),
            pltpu.VMEM((n, 1, width), f32),
            pltpu.VMEM((n, 1, width), f32),
            pltpu.VMEM((n, wide), f32),
            pltpu.VMEM((n, width), f32),
            dma((3,)), dma((ITERS,)), dma((ITERS,)), dma((ITERS,)), dma((ITERS,)), dma((2,)), dma((2,)), dma((2,)),
        ],
        compiler_params=pltpu.CompilerParams(collective_id=0, has_side_effects=True, vmem_limit_bytes=24*2**20),
    )(estimated_returns, chosen_move_ids, previous_eta, trust_region_epsilon)
    pieces = max(rows // 8, 1)
    sample, goal, eta = pl.pallas_call(
        finish,
        name="finish",
        out_shape=(
            jax.ShapeDtypeStruct((rows, columns), f32),
            jax.ShapeDtypeStruct((NACT, width), f32),
            jax.ShapeDtypeStruct((1, LANES), f32),
        ),
        in_specs=[vmem, vmem, vmem, vmem],
        out_specs=(anywhere, anywhere, anywhere),
        scratch_shapes=[pltpu.VMEM((rows, columns), f32), dma((pieces + 2,))],
        compiler_params=pltpu.CompilerParams(vmem_limit_bytes=32 * 2**20),
    )(expo, scale, goal, eta)
    return sample, goal, eta[0, :1]


def solution(mesh):
    n, m = mesh.shape["act"], mesh.shape["rep"]
    return jax.shard_map(
        functools.partial(on_device, n, m),
        mesh=mesh,
        in_specs=(P("act", "rep"), P("act", "rep"), P(), P()),
        out_specs=(P("act", "rep"), P(None, ("rep", "act")), P()),
        check_vma=False,
    )
```

```python
import functools

import jax
import jax.numpy as jnp
from jax import lax
from jax.experimental import pallas as pl
from jax.experimental.pallas import tpu as pltpu
from jax.sharding import PartitionSpec as P

NACT = 18
ITERS = 3
LANES = 128
MESH = pl.DeviceIdType.MESH


def fold_lanes(x):
    total = x[:, :LANES]
    for i in range(1, x.shape[1] // LANES):
        total = total + x[:, i * LANES : (i + 1) * LANES]
    return total


def kernel(
    n, m, q_hbm, ids_hbm, eta_ref, eps_ref,
    expo_hbm, scale_ref, goal_ref, eta_out,
    q, ids, stat_src, stat_dst, pair_src, pair_dst, pair_sent, z_src, z_dst, goal_src, goal_dst, scale_src, scale_dst, delta, parts,
    local_sem, stat_send, stat_recv, pair_send, pair_recv, z_sem, goal_sem, scale_sem,
):
    a, r = lax.axis_index("act"), lax.axis_index("rep")
    me = r * n + a
    devices = n * m
    rows, columns = q.shape
    width = columns // n
    owners, first_owner = n // 2, n // 4
    wide = columns // owners
    is_owner = jnp.logical_and(a >= first_owner, a < first_owner + owners)
    mine = lax.rem(a - first_owner + n, n)
    samples = jnp.float32(rows * n)
    states = jnp.float32(columns * m)

    barrier = pltpu.get_barrier_semaphore()

    def greet(o, c):
        to = lax.rem(me + o, devices)
        pl.semaphore_signal(
            barrier, inc=1, device_id={"act": lax.rem(to, n), "rep": to // n}, device_id_type=MESH
        )
        return c

    lax.fori_loop(1, devices, greet, 0)
    load_q = pltpu.make_async_copy(q_hbm, q, local_sem.at[0])
    load_ids = pltpu.make_async_copy(ids_hbm, ids, local_sem.at[1])
    load_q.start()
    load_ids.start()
    load_q.wait()

    def wide_cols(i):
        return pl.ds(pl.multiple_of(i * wide, LANES), wide)

    def cols(j):
        return pl.ds(pl.multiple_of(j * width, LANES), width)

    def to_peer(src, dst, send, recv, j):
        return pltpu.make_async_remote_copy(
            src_ref=src, dst_ref=dst, send_sem=send, recv_sem=recv,
            device_id={"act": j, "rep": r}, device_id_type=MESH,
        )

    def all_but_one(ref, count, sem):
        some = ref.at[pl.ds(0, count - 1)]
        pltpu.make_async_copy(some, some, sem).wait()

    eta = jnp.full((1, LANES), eta_ref[0], jnp.float32)
    eps = jnp.full((1, LANES), eps_ref[0], jnp.float32)

    def statistics(step, i, inverse):
        c = wide_cols(i)
        if step == 0:
            block = q[:, c]
            top = jnp.max(block, axis=0, keepdims=True)
            shifted = block - top
            q[:, c] = shifted
            stat_src[step, i, 3:4, :] = top
        else:
            shifted = q[:, c]
        expo = jnp.exp(shifted * inverse)
        first = expo * shifted
        stat_src[step, i, 0:1, :] = jnp.sum(expo, axis=0, keepdims=True)
        stat_src[step, i, 1:2, :] = jnp.sum(first, axis=0, keepdims=True)
        stat_src[step, i, 2:3, :] = jnp.sum(first * shifted, axis=0, keepdims=True)

    for step in range(ITERS):
        inverse = 1.0 / eta[:, :1]
        if step == 0:
            lax.fori_loop(0, owners, lambda i, c: (statistics(0, i, inverse), c)[1], 0)
            pl.semaphore_wait(barrier, devices - 1)

        def send(o, c):
            i = lax.rem(a - first_owner + n // 2 + o + n, owners)
            if step > 0:
                statistics(step, i, inverse)

            @pl.when(i + first_owner != a)
            def _():
                to_peer(
                    stat_src.at[step, i], stat_dst.at[step, a], stat_send.at[step], stat_recv.at[step],
                    i + first_owner,
                ).start()

            return c

        lax.fori_loop(0, owners, send, 0)

        @pl.when(is_owner)
        def _():
            stat_dst[step, a] = stat_src[step, mine]
            all_but_one(stat_dst.at[step], n, stat_recv.at[step])
            z_d = stat_dst[step, :, 0, :]
            c1_d = stat_dst[step, :, 1, :]
            c2_d = stat_dst[step, :, 2, :]
            if step == 0:
                top_d = stat_dst[step, :, 3, :]
                gap = top_d - jnp.max(top_d, axis=0, keepdims=True)
                delta[...] = gap
            else:
                gap = delta[...]
            e_d = jnp.exp(gap * inverse)
            z = jnp.sum(e_d * z_d, axis=0, keepdims=True)
            c1 = jnp.sum(e_d * (c1_d + gap * z_d), axis=0, keepdims=True)
            c2 = jnp.sum(e_d * (c2_d + gap * (2.0 * c1_d + gap * z_d)), axis=0, keepdims=True)
            mean = c1 / z
            kl = mean * inverse - jnp.log(z) + jnp.log(samples)
            spread = c2 / z - mean * mean
            pair_src[step, 0:1, :] = fold_lanes(kl)
            pair_src[step, 1:2, :] = fold_lanes(spread)
            slot = r * owners + mine

            def share(o, c):
                for turn in range(m):
                    pltpu.make_async_remote_copy(
                        src_ref=pair_src.at[step], dst_ref=pair_dst.at[step, slot],
                        send_sem=pair_send.at[step], recv_sem=pair_recv.at[step],
                        device_id={"act": lax.rem(a + o, n), "rep": lax.rem(r + turn, m)}, device_id_type=MESH,
                    ).start()
                return c

            lax.fori_loop(1, n, share, 0)
            for turn in range(1, m):
                pltpu.make_async_remote_copy(
                    src_ref=pair_src.at[step], dst_ref=pair_dst.at[step, slot],
                    send_sem=pair_send.at[step], recv_sem=pair_recv.at[step],
                    device_id={"rep": lax.rem(r + turn, m)}, device_id_type=MESH,
                ).start()
            pair_dst[step, slot] = pair_src[step]
            all_but_one(pair_dst.at[step], owners * m, pair_recv.at[step])

        @pl.when(jnp.logical_not(is_owner))
        def _():
            pltpu.make_async_copy(pair_dst.at[step], pair_dst.at[step], pair_recv.at[step]).wait()

        both = jnp.sum(pair_dst[step], axis=0)
        both = jnp.sum(both, axis=1, keepdims=True) / states
        k_mean = jnp.broadcast_to(both[0:1], (1, LANES))
        v_mean = jnp.broadcast_to(both[1:2], (1, LANES))
        change = (eps - k_mean) * eta / (1.0 + v_mean / eta)
        eta = eta * jnp.exp(-jnp.tanh(change))

    inverse = 1.0 / eta[:, :1]
    eta_out[...] = eta

    def weights(j):
        c = cols(j)
        expo = jnp.exp(q[:, c] * inverse)
        q[:, c] = expo
        z_src[j, 0:1, :] = jnp.sum(expo, axis=0, keepdims=True)
        z_src[j, 1:2, :] = stat_src[0, j * width // wide, 3:4, pl.ds(pl.multiple_of(lax.rem(j * width, wide), LANES), width)]

    def send_z(o, c):
        j = lax.rem(a + o, n)
        weights(j)
        to_peer(z_src.at[j], z_dst.at[a], z_sem.at[0], z_sem.at[1], j).start()
        return c

    lax.fori_loop(1, n, send_z, 0)
    weights(a)
    z_dst[a] = z_src[a]
    store_expo = pltpu.make_async_copy(q, expo_hbm, local_sem.at[2])
    store_expo.start()
    load_ids.wait()

    def goals(j):
        c = cols(j)
        for i in range(width // LANES):
            sub = pl.ds(pl.multiple_of(j * width + i * LANES, LANES), LANES)
            expo, moves = q[:, sub], ids[:, sub]
            for k in range(NACT):
                goal_src[j, k : k + 1, i * LANES : (i + 1) * LANES] = jnp.sum(
                    jnp.where(moves == k, expo, 0.0), axis=0, keepdims=True
                )

    def start_goals(o, c):
        j = lax.rem(a + o, n)
        to_peer(goal_src.at[j], goal_dst.at[a], goal_sem.at[0], goal_sem.at[1], j).start()
        return c

    def send_goals(o, c):
        goals(lax.rem(a + o, n))
        return start_goals(o, c)

    lax.fori_loop(1, n // 2, send_goals, 0)
    lax.fori_loop(n // 2, n + 1, lambda o, c: (goals(lax.rem(a + o, n)), c)[1], 0)
    goal_dst[a] = goal_src[a]

    all_but_one(z_dst, n, z_sem.at[1])
    top_d = z_dst[:, 1, :]
    e_d = jnp.exp((top_d - jnp.max(top_d, axis=0, keepdims=True)) * inverse)
    z = jnp.sum(e_d * z_dst[:, 0, :], axis=0, keepdims=True)
    part = e_d / z
    parts[...] = part
    scale_src[:, 0, :] = samples * part

    def send_scale(o, c):
        j = lax.rem(a + o, n)
        to_peer(scale_src.at[j], scale_dst.at[a], scale_sem.at[0], scale_sem.at[1], j).start()
        return c

    lax.fori_loop(1, n, send_scale, 0)
    lax.fori_loop(n // 2, n, start_goals, 0)
    scale_dst[a] = scale_src[a]
    all_but_one(goal_dst, n, goal_sem.at[1])
    goal_ref[...] = lax.fori_loop(
        0, n, lambda d, t: t + parts[pl.ds(d, 1), :] * goal_dst[d], jnp.zeros((NACT, width), jnp.float32)
    )
    all_but_one(scale_dst, n, scale_sem.at[1])

    def place(j, c):
        scale_ref[:, cols(j)] = scale_dst[j]
        return c

    lax.fori_loop(0, n, place, 0)
    for step in range(ITERS):

        @pl.when(is_owner)
        def _():
            all_but_one(stat_src.at[step], owners, stat_send.at[step])
            some = pair_sent.at[pl.ds(0, devices - 1)]
            pltpu.make_async_copy(some, some, pair_send.at[step]).wait()

        @pl.when(jnp.logical_not(is_owner))
        def _():
            pltpu.make_async_copy(stat_src.at[step], stat_src.at[step], stat_send.at[step]).wait()

    all_but_one(z_src, n, z_sem.at[0])
    all_but_one(goal_src, n, goal_sem.at[0])
    all_but_one(scale_src, n, scale_sem.at[0])
    store_expo.wait()


def finish(expo_ref, scale_ref, goal_ref, eta_ref, sample_hbm, goal_hbm, eta_hbm, sample, sem):
    rows, columns = sample.shape
    pieces = sem.shape[0] - 2
    tall = rows // pieces
    copies = [
        pltpu.make_async_copy(goal_ref, goal_hbm, sem.at[pieces]),
        pltpu.make_async_copy(eta_ref, eta_hbm, sem.at[pieces + 1]),
    ]
    for copy in copies:
        copy.start()
    for i in range(pieces):
        at = pl.ds(i * tall, tall)
        sample[at, :] = expo_ref[at, :] * scale_ref[...]
        copy = pltpu.make_async_copy(sample.at[at], sample_hbm.at[at], sem.at[i])
        copy.start()
        copies.append(copy)
    for copy in copies:
        copy.wait()


def on_device(n, m, estimated_returns, chosen_move_ids, previous_eta, trust_region_epsilon):
    rows, columns = estimated_returns.shape
    width = columns // n
    owners = n // 2
    wide = columns // owners
    f32 = jnp.float32
    anywhere = pl.BlockSpec(memory_space=pl.ANY)
    vmem = pl.BlockSpec(memory_space=pltpu.VMEM)
    smem = pl.BlockSpec(memory_space=pltpu.SMEM)
    dma = pltpu.SemaphoreType.DMA
    expo, scale, goal, eta = pl.pallas_call(
        functools.partial(kernel, n, m),
        name="dual",
        out_shape=(
            jax.ShapeDtypeStruct((rows, columns), f32),
            jax.ShapeDtypeStruct((1, columns), f32),
            jax.ShapeDtypeStruct((NACT, width), f32),
            jax.ShapeDtypeStruct((1, LANES), f32),
        ),
        in_specs=[anywhere, anywhere, smem, smem],
        out_specs=(anywhere, vmem, vmem, vmem),
        scratch_shapes=[
            pltpu.VMEM((rows, columns), f32),
            pltpu.VMEM((rows, columns), jnp.int32),
            pltpu.VMEM((ITERS, owners, 4, wide), f32),
            pltpu.VMEM((ITERS, n, 4, wide), f32),
            pltpu.VMEM((ITERS, 2, LANES), f32),
            pltpu.VMEM((ITERS, owners * m, 2, LANES), f32),
            pltpu.VMEM((n * m, 2, LANES), f32),
            pltpu.VMEM((n, 2, width), f32),
            pltpu.VMEM((n, 2, width), f32),
            pltpu.VMEM((n, NACT, width), f32),
            pltpu.VMEM((n, NACT, width), f32),
            pltpu.VMEM((n, 1, width), f32),
            pltpu.VMEM((n, 1, width), f32),
            pltpu.VMEM((n, wide), f32),
            pltpu.VMEM((n, width), f32),
            dma((3,)), dma((ITERS,)), dma((ITERS,)), dma((ITERS,)), dma((ITERS,)), dma((2,)), dma((2,)), dma((2,)),
        ],
        compiler_params=pltpu.CompilerParams(collective_id=0, has_side_effects=True, vmem_limit_bytes=24*2**20),
    )(estimated_returns, chosen_move_ids, previous_eta, trust_region_epsilon)
    pieces = max(rows // 8, 1)
    sample, goal, eta = pl.pallas_call(
        finish,
        name="finish",
        out_shape=(
            jax.ShapeDtypeStruct((rows, columns), f32),
            jax.ShapeDtypeStruct((NACT, width), f32),
            jax.ShapeDtypeStruct((1, LANES), f32),
        ),
        in_specs=[vmem, vmem, vmem, vmem],
        out_specs=(anywhere, anywhere, anywhere),
        scratch_shapes=[pltpu.VMEM((rows, columns), f32), dma((pieces + 2,))],
        compiler_params=pltpu.CompilerParams(vmem_limit_bytes=32 * 2**20),
    )(expo, scale, goal, eta)
    return sample, goal, eta[0, :1]


def solution(mesh):
    n, m = mesh.shape["act"], mesh.shape["rep"]
    return jax.shard_map(
        functools.partial(on_device, n, m),
        mesh=mesh,
        in_specs=(P("act", "rep"), P("act", "rep"), P(), P()),
        out_specs=(P("act", "rep"), P(None, ("rep", "act")), P()),
        check_vma=False,
    )
```
